32 devices in a mesh: dp: 2 (over x), expert: 16 (over z, y, core).
Axes of the slice: x: 2, y: 2, z: 4, core: 2. Of those that a mesh axis runs over, the one named last changes fastest.
Arguments:
- tokens_in: bfloat16 [4096, 2880], P(('dp', 'expert')), may hold values from -6 to 6
- grad_out: bfloat16 [4096, 2880], P(('dp', 'expert')), may hold values from -6 to 6
- expert_ids: int32 [4096, 4], P(('dp', 'expert')), may hold values from 0 to 15, all different within a row; in each aligned block of 128 rows (0 to 127, 128 to 255, ...) at most 40 rows name the same one
- combine_weights: float32 [4096, 4], P(('dp', 'expert')), may hold values from 0.1 to 1
- up_weight: bfloat16 [16, 2880, 1440], P('expert'), may hold values from -0.109375 to 0.109375
- down_weight: bfloat16 [16, 1440, 2880], P('expert'), may hold values from -0.15625 to 0.15625
Outputs:
- grad_input: bfloat16 [4096, 2880], P(('dp', 'expert'))
- grad_up: bfloat16 [16, 2880, 1440], P('expert', 'dp')
- grad_down: bfloat16 [16, 1440, 2880], P('expert', 'dp')
The draws below stay inside these ranges and needn't reach their ends.
Inputs may be any that keep to these rules, and one draw needn't show every extreme that they name: `expert_ids`: each row names 4 different experts; in the rows of one device no expert is named by more than 40 rows, a bound that some block reaches.
All inputs are finite; a program needn't handle non-finite values.
Results may differ from the reference program's by a relative error of at most 0.0064.
Values may be sent and summed in bfloat16 or wider, within the bound.
A program may use at most 192 MiB of HBM per device.

```python
import math
import jax
import jax.numpy as jnp
import numpy as np
from jax import lax

D = 2880
F = 1440
TOPK = 4
TOK_DEV = 128
EXPERTS = 16
CAP = 40
TOKENS = 4096
N_DP = 2
N_EXPERT = 16


def level_of(key, dims, pieces, smallest, top_value):
    factor_of, own = 1.0, jax.random.fold_in(key, 6)
    for dim, blocks in pieces:
        steps = jnp.exp(jax.random.uniform(jax.random.fold_in(own, dim), (blocks,), jnp.float32, smallest / len(pieces), top_value / len(pieces)))
        factor_of = factor_of * jnp.repeat(steps, dims[dim] // blocks).reshape([-1 if axis == dim else 1 for axis in range(len(dims))])
    return factor_of


def deal_out(rng, own, number, rows, amount, top, reach, skew):
    ranking = jax.random.permutation(rng, amount)
    crowded, ordinary = portions_of(amount, rows * top, reach, skew, True), portions_of(amount, rows * top, reach, skew, False)
    places = jnp.arange(amount)

    def named(tallies, turn):
        used = int((tallies > 0).sum())
        fixed = max(1, used // 4)
        passed = fixed + (places - fixed + turn * (used - fixed)) % max(1, amount - fixed)
        return jnp.zeros((amount,), jnp.int32).at[ranking[jnp.where(places < fixed, places, passed)]].set(jnp.asarray(tallies, jnp.int32))

    tallies = jnp.where(number % 4 == 0, named(crowded, number // 4), named(ordinary, number - number // 4 - 1))
    mixed = jax.random.permutation(jax.random.fold_in(own, 3), amount)
    source_of, taker = mixed[0:amount // 2 * 2:2], mixed[1:amount // 2 * 2:2]
    margin = jnp.minimum(tallies[source_of] - 1, reach - tallies[taker]) // 2
    margin = jnp.where((source_of == ranking[0]) | (taker == ranking[0]) | (tallies[taker] == 0), 0, jnp.maximum(margin, 0))
    passed = jax.random.randint(jax.random.fold_in(own, 4), (amount // 2,), 0, 1 << 20) % (margin + 1)
    tallies = tallies.at[source_of].add(-passed).at[taker].add(passed)
    labels = jnp.searchsorted(jnp.cumsum(tallies), jnp.arange(rows * top), side="right").astype(jnp.int32)
    table = labels.reshape(top, rows).T
    table = table[jax.random.permutation(jax.random.fold_in(own, 1), rows)]
    turn = jax.random.randint(jax.random.fold_in(own, 2), (rows, 1), 0, top)
    return jnp.take_along_axis(table, (jnp.arange(top)[None, :] + turn) % top, axis=1)


def portions_of(amount, total, reach, skew, full):
    portions = [(1 << 20) // math.isqrt(standing ** skew) + 1 for standing in range(1, amount + 1)]
    largest = reach if full else min(reach, max(-(-total // amount), total * portions[0] // sum(portions)))
    least = 1 if total - largest >= amount - 1 else 0
    counts, surplus = [largest] + [least] * (amount - 1), total - largest - least * (amount - 1)
    while surplus > 0:
        movable = [i for i in range(1, amount) if counts[i] < largest] or [i for i in range(1, amount) if counts[i] < reach]
        mass, remaining = sum([portions[i] for i in movable]), surplus
        for i in movable:
            extra = min(reach - counts[i], max(1, remaining * portions[i] // mass), surplus)
            counts[i] = counts[i] + extra
            surplus = surplus - extra
    return np.array(counts)


def bell_draw(own_key, dims, deviation, bound, shards=(), kind=jnp.bfloat16):
    array = jax.random.normal(own_key, dims, jnp.float32) * deviation
    if len(shards) > 0:
        array = level_of(own_key, dims, shards, -0.22, 0.18) * array
    return jnp.clip(array, min=-bound, max=bound).astype(kind)


def setup_inputs(seed: int = 0) -> dict:
    key_list = jax.random.split(jax.random.key(seed), 7)
    tokens_in = bell_draw(key_list[0], (TOKENS, D), 1.0, 6.0, ((0, 32),))
    grad_out = bell_draw(key_list[1], (TOKENS, D), 1.0, 6.0, ((0, 32),))
    expert_ids_keys = jax.random.split(jax.random.fold_in(key_list[2], 1), TOKENS // TOK_DEV)
    expert_ids_turns = jax.random.permutation(jax.random.fold_in(key_list[2], 3), TOKENS // TOK_DEV)
    expert_ids = jax.vmap(lambda own, number: deal_out(jax.random.fold_in(key_list[2], 2), own, number, TOK_DEV, EXPERTS, TOPK, CAP, 1))(expert_ids_keys, expert_ids_turns).reshape((TOKENS, TOPK))
    combine_weights = jnp.clip(jnp.exp(math.log(1.0) - 2.3025851 * jax.random.uniform(key_list[3], (TOKENS, TOPK), jnp.float32) ** level_of(key_list[3], (TOKENS, TOPK), ((0, 32),), -0.2, 0.2)), 0.1, 1.0)
    up_weight = bell_draw(key_list[4], (EXPERTS, D, F), D ** -0.5, 0.109375, ((0, 16),))
    down_weight = bell_draw(key_list[5], (EXPERTS, F, D), F ** -0.5, 0.15625, ((0, 16),))
    return dict(tokens_in=tokens_in, grad_out=grad_out, expert_ids=expert_ids, combine_weights=combine_weights, up_weight=up_weight, down_weight=down_weight)


def silu_parts(preact):
    logistic = jax.nn.sigmoid(preact)
    return preact * logistic, logistic * (1.0 + preact * (1.0 - logistic))


def reference(tokens_in, grad_out, expert_ids, combine_weights, up_weight, down_weight):
    model_width = tokens_in.shape[1]
    devices_all = N_DP * N_EXPERT
    block_rows = TOK_DEV * TOPK
    per_expert = devices_all * CAP
    routed = TOKENS * TOPK
    flat_ids = expert_ids.reshape(devices_all, block_rows)
    one_hot = (flat_ids[:, :, None] == jnp.arange(EXPERTS, dtype=jnp.int32)[None, None, :]).astype(jnp.int32)
    slot_rank = jnp.sum((jnp.cumsum(one_hot, axis=1) - one_hot) * one_hot, axis=2)
    source_dev = jnp.arange(devices_all, dtype=jnp.int32)[:, None]
    position = (flat_ids * per_expert + source_dev * CAP + slot_rank).reshape(-1).astype(jnp.int32)
    slot_table = jnp.full((EXPERTS * per_expert,), routed, jnp.int32).at[position].set(jnp.arange(routed, dtype=jnp.int32))
    padded_x = jnp.concatenate([tokens_in, jnp.zeros((1, model_width), tokens_in.dtype)], axis=0)
    padded_dy = jnp.concatenate([grad_out, jnp.zeros((1, model_width), grad_out.dtype)], axis=0)
    padded_weight = jnp.concatenate([combine_weights.reshape(-1), jnp.zeros((1,), combine_weights.dtype)], axis=0)

    def one_expert(operands):
        rows_idx, w_up, w_down = operands
        source_token = rows_idx // TOPK
        rows_x = padded_x[source_token]
        rows_grad = (padded_weight[rows_idx][:, None] * padded_dy[source_token].astype(jnp.float32)).astype(jnp.bfloat16)
        preact = jnp.dot(rows_x, w_up, preferred_element_type=jnp.float32)
        activated, slope = silu_parts(preact)
        activated = activated.astype(jnp.bfloat16)
        grad_act = jnp.dot(rows_grad, w_down.T, preferred_element_type=jnp.float32)
        grad_pre = (grad_act * slope).astype(jnp.bfloat16)
        grad_rows = jnp.dot(grad_pre, w_up.T, preferred_element_type=jnp.float32).astype(jnp.bfloat16)
        grad_upper = jnp.dot(rows_x.T, grad_pre, preferred_element_type=jnp.float32).astype(jnp.bfloat16)
        grad_lower = jnp.dot(activated.T, rows_grad, preferred_element_type=jnp.float32).astype(jnp.bfloat16)
        return grad_rows, grad_upper, grad_lower

    grad_rows, grad_up, grad_down = lax.map(one_expert, (slot_table.reshape(EXPERTS, per_expert), up_weight, down_weight))
    picked = grad_rows.reshape(-1, model_width)[position].reshape(TOKENS, TOPK, model_width)
    grad_input = jnp.sum(picked.astype(jnp.float32), axis=1).astype(jnp.bfloat16)
    return grad_input, grad_up, grad_down
```

```python
import jax
import jax.numpy as jnp
from jax import lax
from jax.sharding import PartitionSpec as P


def silu_parts(preact):
    logistic = jax.nn.sigmoid(preact)
    return (preact * logistic, logistic * (1.0 + preact * (1.0 - logistic)))


def contract_rows(left, right):
    return lax.dot_general(
        left, right, (((0,), (0,)), ((), ())), preferred_element_type=jnp.float32
    )


def contract_cols(left, right):
    return lax.dot_general(
        left, right, (((1,), (1,)), ((), ())), preferred_element_type=jnp.float32
    )


def other_replica(value):
    pairs = lax.axis_size("dp")
    return lax.ppermute(value, "dp", [(i, (i + 1) % pairs) for i in range(pairs)])


def slots_of(expert_ids, combine_weights, experts_all, capacity):
    token_count, top_count = expert_ids.shape
    hits = expert_ids[:, :, None] == jnp.arange(experts_all, dtype=jnp.int32)[None, None, :]
    chosen = jnp.any(hits, axis=1).astype(jnp.bfloat16)
    token_index = jnp.arange(token_count, dtype=jnp.int32)
    earlier = (token_index[None, :] < token_index[:, None]).astype(jnp.bfloat16)
    rank = jnp.dot(earlier, chosen, preferred_element_type=jnp.float32).astype(jnp.int32)
    slot_rank = jnp.sum(jnp.where(hits, rank[:, None, :], 0), axis=2)
    position = expert_ids * capacity + slot_rank
    slot = jnp.arange(experts_all * capacity, dtype=jnp.int32)
    taken = jnp.zeros((token_count, experts_all * capacity), jnp.float32)
    weight = taken
    for k in range(top_count):
        match = position[:, k][:, None] == slot[None, :]
        taken = jnp.where(match, 1.0, taken)
        weight = jnp.where(match, combine_weights[:, k][:, None], weight)
    return taken.astype(jnp.bfloat16), jnp.sum(weight, axis=0)


def local(tokens_in, grad_out, expert_ids, combine_weights, up_weight, down_weight):
    token_count, _ = tokens_in.shape
    top_count = expert_ids.shape[1]
    experts_all = lax.axis_size("expert") * up_weight.shape[0]
    capacity = 5 * token_count * top_count // (4 * experts_all)
    place, slot_weight = slots_of(expert_ids, combine_weights, experts_all, capacity)
    w_up = up_weight[0]
    w_down = down_weight[0]
    replica = lax.axis_index("dp")

    def halves(value):
        half = value.shape[1] // 2
        low, high = value[:, :half], value[:, half:]
        first = replica == 0
        return jnp.where(first, low, high), jnp.where(first, high, low)

    def to_experts(rows):
        return lax.all_to_all(rows, "expert", split_axis=0, concat_axis=0, tiled=True)

    send_grad = (contract_rows(place, grad_out) * slot_weight[:, None]).astype(jnp.bfloat16)
    send_x = contract_rows(place, tokens_in).astype(jnp.bfloat16)
    rows_grad = to_experts(send_grad)
    other_grad = other_replica(rows_grad)
    rows_x = to_experts(send_x)
    grad_act = lax.optimization_barrier(contract_cols(rows_grad, w_down))
    keep_x, give_x = halves(rows_x)
    other_x = other_replica(give_x)
    preact = jnp.dot(rows_x, w_up, preferred_element_type=jnp.float32)
    activated, slope = silu_parts(preact)
    activated = activated.astype(jnp.bfloat16)
    grad_pre = (grad_act * slope).astype(jnp.bfloat16)
    keep_act, give_act = halves(activated)
    other_act = other_replica(give_act)
    other_pre = other_replica(grad_pre)
    grad_rows = contract_cols(grad_pre, w_up).astype(jnp.bfloat16)
    returned = to_experts(grad_rows)
    grad_down = contract_rows(keep_act, rows_grad) + contract_rows(other_act, other_grad)
    grad_up = contract_rows(keep_x, grad_pre) + contract_rows(other_x, other_pre)
    grad_input = jnp.dot(place, returned, preferred_element_type=jnp.float32).astype(jnp.bfloat16)
    return (grad_input, grad_up.astype(jnp.bfloat16)[None], grad_down.astype(jnp.bfloat16)[None])


def solution(mesh):
    return jax.shard_map(
        local,
        mesh=mesh,
        in_specs=(
            P(("dp", "expert"), None),
            P(("dp", "expert"), None),
            P(("dp", "expert"), None),
            P(("dp", "expert"), None),
            P("expert", None, None),
            P("expert", None, None),
        ),
        out_specs=(P(("dp", "expert"), None), P("expert", "dp", None), P("expert", "dp", None)),
        check_vma=False,
    )
```
